32 devices in a mesh: py: 4 (over y, x), px: 4 (over z), pz: 2 (over core).
Axes of the slice: x: 2, y: 2, z: 4, core: 2. Of those that a mesh axis runs over, the one named last changes fastest.
Arguments:
- field_now: float32 [16, 512, 64, 128], P('py', 'px', 'pz'), may hold values from 0.5 to 2
- earlier: float32 [16, 512, 64, 128], P('py', 'px', 'pz'), may hold values from 0.2 to 1.8
- speed_square: float32 [16, 512, 64, 128], P('py', 'px', 'pz'), may hold values from 0.05 to 0.3
Outputs:
- anomaly: float32 [16, 512, 64, 128], P('py', 'px', 'pz')
- field_now_end: float32 [16, 512, 64, 128], P('py', 'px', 'pz')
The draws below stay inside these ranges and needn't reach their ends.
All inputs are finite; a program needn't handle non-finite values.
Results may differ from the reference program's by a relative error of at most 0.00002.
Values sent between devices are 32-bit elements; how exact they have to be, the bound alone decides.
No kernel may reach another device: no remote copies, remote signals or barrier semaphores. Data moves between devices by JAX's collectives and lax.ppermute only.
A program may use at most 128 MiB of HBM per device.

```python
import jax
import jax.numpy as jnp
from jax import lax

GRID_J = 16
GRID_I = 512
GRID_K = 64
LEVELS = 128
STEPS = 4


def shard_levels(key, extent, pieces, smallest, high):
    factor_of, own = 1.0, jax.random.fold_in(key, 6)
    for dim, blocks in pieces:
        draws = jnp.exp(jax.random.uniform(jax.random.fold_in(own, dim), (blocks,), jnp.float32, smallest / len(pieces), high / len(pieces)))
        factor_of = factor_of * jnp.repeat(draws, extent[dim] // blocks).reshape([-1 if axis == dim else 1 for axis in range(len(extent))])
    return factor_of


def setup_inputs(seed: int = 0) -> dict:
    streams_of = jax.random.split(jax.random.key(seed), 4)
    return {
        "field_now": jnp.clip(0.5 + 1.5 * jax.random.uniform(streams_of[0], (GRID_J, GRID_I, GRID_K, LEVELS), jnp.float32) ** shard_levels(streams_of[0], (GRID_J, GRID_I, GRID_K, LEVELS), ((0, 4), (1, 4), (2, 2)), -0.2, 0.2), 0.5, 2.0),
        "earlier": jnp.clip(0.2 + 1.5999999 * jax.random.uniform(streams_of[1], (GRID_J, GRID_I, GRID_K, LEVELS), jnp.float32) ** shard_levels(streams_of[1], (GRID_J, GRID_I, GRID_K, LEVELS), ((0, 4), (1, 4), (2, 2)), -0.2, 0.2), 0.2, 1.8),
        "speed_square": jnp.clip(0.05 + 0.25 * jax.random.uniform(streams_of[2], (GRID_J, GRID_I, GRID_K, LEVELS), jnp.float32) ** shard_levels(streams_of[2], (GRID_J, GRID_I, GRID_K, LEVELS), ((0, 4), (1, 4), (2, 2)), -0.2, 0.2), 0.05, 0.3),
    }


def inner_cells(values, dims):
    for dim in dims:
        values = lax.slice_in_dim(values, 1, values.shape[dim] - 1, axis=dim)
    return values

def side_cells(values, dim, start, dims):
    others = [other for other in dims if other != dim]
    values = inner_cells(values, others)
    return lax.slice_in_dim(values, start, start + values.shape[dim] - 2, axis=dim)

def advance(padded, before, speed_square):
    middle = inner_cells(padded, (0, 1, 2))
    lower = [side_cells(padded, dim, 0, (0, 1, 2)) for dim in (0, 1, 2)]
    upper = [side_cells(padded, dim, 2, (0, 1, 2)) for dim in (0, 1, 2)]
    spread = lower[0] + upper[0] + lower[1] + upper[1] + lower[2] + upper[2] - 6.0 * middle
    return 2.0 * middle - before + speed_square * spread

def reference(field_now, earlier, speed_square):
    for step in range(STEPS):
        later = advance(jnp.pad(field_now, ((1, 1), (1, 1), (1, 1), (0, 0)), mode='constant'), earlier, speed_square)
        earlier, field_now = (field_now, later)
    line_mean = lax.optimization_barrier(jnp.mean(field_now, axis=1, keepdims=True))
    centred = field_now - line_mean
    line_variance = lax.optimization_barrier(jnp.mean(centred * centred, axis=1, keepdims=True))
    anomaly = centred * lax.rsqrt(line_variance + 0.0001)
    return (anomaly, field_now)
```

```python
import math
from functools import partial

import jax
import jax.numpy as jnp
from jax import lax
from jax.experimental import pallas as pl
from jax.experimental.pallas import tpu as pltpu
from jax.sharding import PartitionSpec as P

STEPS = 4
CHUNKS = 2
GUESS = 1.0
PARAMS = pltpu.CompilerParams(vmem_limit_bytes=60 * 1024 * 1024)


def spec(block, index):
    return pl.BlockSpec(block, lambda g, index=index: index)


def whole(array):
    return (array, spec(array.shape, (0,) * array.ndim))


def sweep(center, below, above, prev, speed, row_lo, row_hi, edge_lo, edge_hi, start, put, stats):
    rows, nk, levels = center.shape
    place = lax.broadcasted_iota(jnp.int32, (nk, levels), 0)
    first, last = place == 0, place == nk - 1

    def one(i, behind, here, ahead, sums):
        kl = jnp.broadcast_to(edge_lo[pl.ds(start + i, 1), :], (nk, levels))
        kh = jnp.broadcast_to(edge_hi[pl.ds(start + i, 1), :], (nk, levels))
        left = jnp.where(first, kl, pltpu.roll(here, 1, 0))
        right = jnp.where(last, kh, pltpu.roll(here, nk - 1, 0))
        spread = (below(i) + above(i)) + (behind + ahead) + (left + right) - 6.0 * here
        new = 2.0 * here - prev[i] + speed[i] * spread
        put(i, new)
        if stats:
            moved = new - GUESS
            sums = (sums[0] + moved, sums[1] + moved * moved)
        return sums

    zero = jnp.zeros((nk, levels), jnp.float32)

    def step(i, carry):
        behind, here, sums = carry
        ahead = center[i + 1]
        sums = one(i, behind, here, ahead, sums)
        return here, ahead, sums

    behind, here, sums = lax.fori_loop(
        0, rows - 1, step, (row_lo[0], center[0], (zero, zero) if stats else ()), unroll=2
    )
    return one(rows - 1, behind, here, row_hi[0], sums)


def run(body, views, out_shape, out_specs, grid, aliases=None, smem=None, name=None):
    arrays = [v[0] for v in views]
    specs = [v[1] for v in views]
    return pl.pallas_call(
        body,
        grid=(grid,),
        in_specs=specs,
        out_specs=out_specs,
        out_shape=out_shape,
        input_output_aliases=aliases or {},
        compiler_params=PARAMS,
        name=name,
    )(*arrays)


def either(count, q, pid, fn):
    if count == 1:
        fn()
    else:
        pl.when(pid == q)(fn)


def shards(field_now, earlier, speed_square):
    nj, ni, nk, levels = field_now.shape
    ic = ni // CHUNKS
    inner = nj - 2
    f32 = jnp.float32
    py, px, pz = (lax.axis_size(a) for a in ("py", "px", "pz"))
    row = math.isqrt(py)
    turns = [p for p in range(py - 1) if (p + 1) % row == 0] if row > 1 and row * row == py else []
    rank = lax.axis_index("py")
    relay_hi = (rank % row == row - 1) & (rank < py - 1) if turns else rank < 0
    relay_lo = (rank % row == 0) & (rank > 0) if turns else rank < 0
    flags = jnp.stack([relay_lo, relay_hi]).astype(jnp.int32)
    flag_view = (flags, pl.BlockSpec(memory_space=pltpu.SMEM))

    def up(x, axis, pairs):
        return lax.ppermute(x, axis, pairs)

    def chain(n):
        return [(p, p + 1) for p in range(n - 1)], [(p + 1, p) for p in range(n - 1)]

    ups, downs = chain(py)

    def send(lo, hi, c):
        if c == CHUNKS - 1 and turns:
            outward = up(
                jnp.where(relay_hi, hi, lo), "py",
                [(p, p + row) for p in turns] + [(p + 1, p + 1 - row) for p in turns],
            )
            below = up(hi, "py", [(p, p + 1) for p in range(py - 1) if p not in turns])
            above = up(lo, "py", [(p + 1, p) for p in range(py - 1) if p not in turns])
            inward = up(
                outward, "py",
                [(p + row, p + 1) for p in turns] + [(p + 1 - row, p) for p in turns],
            )
            return below, above, inward
        return up(hi, "py", ups), up(lo, "py", downs), None

    def view0(array, j, c):
        return (array, spec((None, ic, nk, levels), (j, c, 0, 0)))

    pieces = [[[view0(field_now, j, c) for c in range(CHUNKS)] for j in range(nj)]]
    before = [[view0(earlier, j, c) for c in range(CHUNKS)] for j in range(nj)]
    speeds = [[view0(speed_square, j, c) for c in range(CHUNKS)] for j in range(nj)]

    def cut(j, c):
        return lax.slice(field_now, (j, c * ic, 0, 0), (j + 1, (c + 1) * ic, nk, levels))[0]

    ghosts = [send(cut(0, c), cut(nj - 1, c), c) for c in range(CHUNKS)]
    rows = (field_now[:, 0], field_now[:, ni - 1])
    cols = (field_now[:, :, 0], field_now[:, :, nk - 1])
    pxu, pxd = chain(px)
    pzu, pzd = chain(pz)
    now = pieces[0]
    for step in range(STEPS):
        final = step == STEPS - 1
        row_lo, row_hi = up(rows[1], "px", pxu), up(rows[0], "px", pxd)
        col_lo, col_hi = up(cols[1], "pz", pzu), up(cols[0], "pz", pzd)

        def row_views(j, c):
            if c == 0:
                lo = (row_lo, spec((1, nk, levels), (j, 0, 0)))
            else:
                lo = last_row(now[j][c - 1])
            if c == CHUNKS - 1:
                hi = (row_hi, spec((1, nk, levels), (j, 0, 0)))
            else:
                hi = first_row(now[j][c + 1])
            return lo, hi

        def one_row(view, i):
            array, bs = view
            at = bs.index_map(0)
            if array.ndim == 4:
                return (array, spec((None, 1, nk, levels), (at[0], at[1] * ic + i, 0, 0)))
            return (array, spec((1, nk, levels), (i, 0, 0)))

        def last_row(view):
            return one_row(view, ic - 1)

        def first_row(view):
            return one_row(view, 0)

        views = [v for j in range(nj) for v in now[j]]
        views += [v for j in range(1, nj - 1) for v in before[j]]
        views += [v for j in range(1, nj - 1) for v in speeds[j]]
        views += [whole(row_lo), whole(row_hi), whole(col_lo), whole(col_hi)]

        def inner_body(*refs, final=final):
            n = nj * CHUNKS
            m = inner * CHUNKS
            u = refs[:n]
            e = refs[n:n + m]
            s = refs[n + m:n + 2 * m]
            rl, rh, cl, ch = refs[n + 2 * m:n + 2 * m + 4]
            out, extra = refs[n + 2 * m + 4:]
            pid = pl.program_id(0)
            for q in range(inner):
                j = q + 1

                def work(q=q, j=j):
                    total = None
                    for c in range(CHUNKS):
                        low, high = u[(j - 1) * CHUNKS + c], u[(j + 1) * CHUNKS + c]
                        lo = rl.at[pl.ds(j, 1)] if c == 0 else u[j * CHUNKS + c - 1].at[pl.ds(ic - 1, 1)]
                        hi = rh.at[pl.ds(j, 1)] if c == CHUNKS - 1 else u[j * CHUNKS + c + 1].at[pl.ds(0, 1)]

                        def put(i, new, c=c):
                            out[0, c * ic + i] = new
                            if not final:
                                extra[0, 0, pl.ds(c * ic + i, 1), :] = new[0:1]
                                extra[0, 1, pl.ds(c * ic + i, 1), :] = new[nk - 1:nk]

                        sums = sweep(
                            u[j * CHUNKS + c], lambda i, r=low: r[i], lambda i, r=high: r[i],
                            e[q * CHUNKS + c], s[q * CHUNKS + c], lo, hi,
                            cl.at[j], ch.at[j], c * ic, put, final,
                        )
                        if final:
                            total = sums if total is None else (total[0] + sums[0], total[1] + sums[1])
                    if final:
                        extra[0, 0] = total[0]
                        extra[0, 1] = total[1]

                either(inner, q, pid, work)

        if final:
            out_shape = [
                jax.ShapeDtypeStruct((nj, ni, nk, levels), f32),
                jax.ShapeDtypeStruct((inner, 2, nk, levels), f32),
            ]
            out_specs = [
                pl.BlockSpec((1, ni, nk, levels), lambda g: (g + 1, 0, 0, 0)),
                pl.BlockSpec((1, 2, nk, levels), lambda g: (g, 0, 0, 0)),
            ]
        else:
            out_shape = [
                jax.ShapeDtypeStruct((inner, ni, nk, levels), f32),
                jax.ShapeDtypeStruct((inner, 2, ni, levels), f32),
            ]
            out_specs = [
                pl.BlockSpec((1, ni, nk, levels), lambda g: (g, 0, 0, 0)),
                pl.BlockSpec((1, 2, ni, levels), lambda g: (g, 0, 0, 0)),
            ]
        mid, mid_extra = run(inner_body, views, out_shape, out_specs, inner, name=f"inner{step}")
        end = mid if final else None

        edge_out, edge_extra, new_ghosts = [], [], []
        for c in range(CHUNKS):
            below, above, relayed = ghosts[c]
            views = [flag_view]
            for j, near in ((0, 1), (nj - 1, nj - 2)):
                lo, hi = row_views(j, c)
                views += [now[j][c], now[near][c], before[j][c], speeds[j][c], lo, hi]
            views += [whole(below), whole(above), whole(col_lo), whole(col_hi)]
            if relayed is not None:
                views.append(whole(relayed))
            if final:
                views.append((end, pl.BlockSpec(memory_space=pl.ANY)))

            def outer_body(*refs, c=c, final=final, relay=relayed is not None):
                flag = refs[0]
                per = [refs[1:7], refs[7:13]]
                below, above, cl, ch = refs[13:17]
                relayed = refs[17] if relay else None
                outs = refs[17 + relay + final:]
                pid = pl.program_id(0)
                for q in range(2):
                    center, near, e, s, lo, hi = per[q]
                    ghost = (below, above)[q]

                    def work(q=q, center=center, near=near, e=e, s=s, lo=lo, hi=hi, ghost=ghost):
                        use = flag[q] > 0

                        def outside(i):
                            if relay:
                                return jnp.where(use, relayed[i], ghost[i])
                            return ghost[i]

                        extra = outs[-1]

                        def put(i, new):
                            if final:
                                outs[0][0, i] = new
                            else:
                                outs[q][i] = new
                                extra[q, 0, pl.ds(i, 1), :] = new[0:1]
                                extra[q, 1, pl.ds(i, 1), :] = new[nk - 1:nk]

                        j = q * (nj - 1)
                        sums = sweep(
                            center, outside, lambda i: near[i], e, s, lo, hi,
                            cl.at[j], ch.at[j], c * ic, put, final,
                        )
                        if final:
                            extra[0, 0] = sums[0]
                            extra[0, 1] = sums[1]

                    either(2 if final else 1, q, pid, work)

            if final:
                end, extra = run(
                    outer_body, views,
                    [
                        jax.ShapeDtypeStruct((nj, ni, nk, levels), f32),
                        jax.ShapeDtypeStruct((2, 2, nk, levels), f32),
                    ],
                    [
                        pl.BlockSpec((1, ic, nk, levels), lambda g, c=c: (g * (nj - 1), c, 0, 0)),
                        pl.BlockSpec((1, 2, nk, levels), lambda g: (g, 0, 0, 0)),
                    ],
                    2, aliases={len(views) - 1: 0}, name=f"outer{step}_{c}",
                )
                edge_extra.append(extra)
            else:
                lo, hi, extra = run(
                    outer_body, views,
                    [jax.ShapeDtypeStruct((ic, nk, levels), f32)] * 2
                    + [jax.ShapeDtypeStruct((2, 2, ic, levels), f32)],
                    [spec((ic, nk, levels), (0, 0, 0))] * 2 + [spec((2, 2, ic, levels), (0, 0, 0, 0))],
                    1, name=f"outer{step}_{c}",
                )
                edge_out.append((lo, hi))
                edge_extra.append(extra)
                new_ghosts.append(send(lo, hi, c))
        if not final:
            planes = [[(edge_out[c][0], spec((ic, nk, levels), (0, 0, 0))) for c in range(CHUNKS)]]
            planes += [[view0(mid, q, c) for c in range(CHUNKS)] for q in range(inner)]
            planes += [[(edge_out[c][1], spec((ic, nk, levels), (0, 0, 0))) for c in range(CHUNKS)]]
            rows = tuple(
                jnp.concatenate([edge_out[c][0][i:i + 1], mid[:, f], edge_out[c][1][i:i + 1]], axis=0)
                for c, i, f in ((0, 0, 0), (CHUNKS - 1, ic - 1, ni - 1))
            )
            cols = tuple(
                jnp.concatenate(
                    [
                        jnp.concatenate([x[0:1, side] for x in edge_extra], axis=1),
                        mid_extra[:, side],
                        jnp.concatenate([x[1:2, side] for x in edge_extra], axis=1),
                    ],
                    axis=0,
                )
                for side in range(2)
            )
            before, now, ghosts = now, planes, new_ghosts

    count = ni * px

    def totals(x):
        return jnp.sum(lax.all_gather(x, "px", axis=0), axis=0)

    def scaled_body(x, st, *rest):
        out = rest[-1]
        shift = st[0, 0] / count
        scale = lax.rsqrt(st[0, 1] / count - shift * shift + 0.0001)
        mean = GUESS + shift

        def step(i, carry):
            out[0, i] = (x[0, i] - mean) * scale
            return carry

        lax.fori_loop(0, x.shape[1], step, 0, unroll=4)

    def scaled(planes, place, stats, onto, source, name):
        half = ni // 2
        block = pl.BlockSpec((1, half, nk, levels), lambda g: (place(g // 2), g % 2, 0, 0))
        views = [(source, block), (stats, pl.BlockSpec((1, 2, nk, levels), lambda g: (g // 2, 0, 0, 0)))]
        if onto is not None:
            views.append((onto, pl.BlockSpec(memory_space=pl.ANY)))
        return run(
            scaled_body, views, jax.ShapeDtypeStruct((nj, ni, nk, levels), f32), block, planes * 2,
            aliases={2: 0} if onto is not None else None, name=name,
        )

    inner_total = totals(mid_extra)
    anomaly = scaled(inner, lambda p: p + 1, inner_total, None, mid, "scale_inner")
    outer_total = totals(sum(edge_extra[1:], edge_extra[0]))
    anomaly = scaled(2, lambda p: p * (nj - 1), outer_total, anomaly, end, "scale_outer")
    return (anomaly, end)


def solution(mesh):
    return jax.shard_map(
        shards,
        mesh=mesh,
        in_specs=(P("py", "px", "pz", None),) * 3,
        out_specs=(P("py", "px", "pz", None),) * 2,
        check_vma=False,
    )
```
